128 devices in a mesh: grp: 2 (over x_hi), fsdp: 8 (over x_lo, z), tp: 8 (over y, core).
Axes of the slice: x: 4 (x_hi: 2, x_lo: 2; x = x_hi * 2 + x_lo), y: 4, z: 4, core: 2. Of those that a mesh axis runs over, the one named last changes fastest.
Arguments:
- learn_hidden: bfloat16 [16384, 14336], P(('grp', 'fsdp'), 'tp'), may hold values from -6 to 6
- learn_cotangent: bfloat16 [16384, 4096], P(('grp', 'fsdp')), may hold values from -0.0625 to 0.0625
- master_weight: float32 [4096, 14336], P(('grp', 'fsdp'), 'tp'), may hold values from -0.046875 to 0.046875
- momentum: float32 [4096, 14336], P(('grp', 'fsdp'), 'tp'), may hold values from -6 to 6
- roll_hidden: bfloat16 [512, 14336], P(('grp', 'fsdp'), 'tp'), may hold values from -6 to 6
Outputs:
- momentum_new: float32 [4096, 14336], P(('grp', 'fsdp'), 'tp')
- roll_out: bfloat16 [512, 4096], P(('grp', 'fsdp'))
The draws below stay inside these ranges and needn't reach their ends.
All inputs are finite; a program needn't handle non-finite values.
Results may differ from the reference program's by a relative error of at most 0.015.
Values may be sent and summed in bfloat16 or wider, within the bound.
No kernel may reach another device: no remote copies, remote signals or barrier semaphores. Data moves between devices by JAX's collectives and lax.ppermute only.
A program may use at most 128 MiB of HBM per device.

```python
import jax
import jax.numpy as jnp
from jax import lax

D = 4096
FF = 14336
TOK_DEV = 1024
TOKENS = 16384
ROLLS = 512
N_GRP = 2
N_FSDP = 8


def with_spikes(drawn, rng, source, target, shards_of, factor):
    owner, partner = [(jnp.arange(drawn.shape[position]) // (drawn.shape[position] // shards_of)).reshape([-1 if axis == position else 1 for axis in range(drawn.ndim)]) for position in (source, target)]
    chosen = jax.random.permutation(rng, shards_of)[partner]
    strong = (owner == chosen) | (owner == (partner + shards_of // 2) % shards_of)
    return jnp.where(strong, factor * drawn, drawn)


def steps_of(stream_key, extent, pieces, smallest, top_value):
    def one(dim, parts):
        draws = jax.random.uniform(jax.random.fold_in(jax.random.fold_in(stream_key, 6), dim), (parts,), jnp.float32, smallest / len(pieces), top_value / len(pieces))
        return jnp.repeat(jnp.exp(draws), extent[dim] // parts).reshape((-1,) + (1,) * (len(extent) - dim - 1))

    factor_of = one(*pieces[0])
    for cut in pieces[1:]:
        factor_of = factor_of * one(*cut)
    return factor_of


def bell_draw(key, shape, spread, limit, pieces=(), held_as=jnp.bfloat16):
    values = jax.random.normal(key, shape, jnp.float32) * spread
    if len(pieces) > 0:
        values = steps_of(key, shape, pieces, -0.22, 0.18) * values
    return jnp.clip(values, min=-limit, max=limit).astype(held_as)


def noise_with(stream_key, dims, deviation, most, split, heavy, held_as=jnp.bfloat16):
    entries = deviation * jax.random.normal(stream_key, dims, jnp.float32)
    if split:
        entries = entries * steps_of(stream_key, dims, split, -0.22, 0.18)
    return jnp.clip(with_spikes(entries, jax.random.fold_in(stream_key, 3), *heavy), -most, most).astype(held_as)


def setup_inputs(seed: int = 0) -> dict:
    streams_of = jax.random.split(jax.random.key(seed), 6)
    return {
        "learn_hidden": bell_draw(streams_of[0], (TOKENS, FF), 1.0, 6.0, ((0, 16), (1, 8))),
        "learn_cotangent": noise_with(streams_of[1], (TOKENS, D), (TOKENS ** -0.5), 0.0625, ((0, 16),), (0, 1, 16, 2.0)),
        "master_weight": bell_draw(streams_of[2], (D, FF), FF ** -0.5, 0.046875, ((0, 16), (1, 8)), jnp.float32),
        "momentum": bell_draw(streams_of[3], (D, FF), 1.0, 6.0, ((0, 16), (1, 8)), jnp.float32),
        "roll_hidden": bell_draw(streams_of[4], (ROLLS, FF), 1.0, 6.0, ((0, 16), (1, 8))),
    }


MOMENTUM = 0.9
LEARN_RATE = 0.002


def reference(learn_hidden, learn_cotangent, master_weight, momentum, roll_hidden):
    groups = N_GRP * N_FSDP
    cot_groups = learn_cotangent.reshape(groups, TOK_DEV, D)
    hid_groups = learn_hidden.reshape(groups, TOK_DEV, FF)

    def add_group(total, pair):
        cot, hid = pair
        term = lax.dot_general(cot, hid, (((0,), (0,)), ((), ())), preferred_element_type=jnp.float32)
        rounded = lax.optimization_barrier(term.astype(jnp.bfloat16))
        return total + rounded.astype(jnp.float32), None

    grad, _ = lax.scan(add_group, jnp.zeros((D, FF), jnp.float32), (cot_groups, hid_groups))
    momentum_new = MOMENTUM * momentum + grad
    rollout_weight = (master_weight - LEARN_RATE * momentum_new).astype(jnp.bfloat16)
    roll_out = lax.dot_general(roll_hidden, rollout_weight, (((1,), (1,)), ((), ())), preferred_element_type=jnp.float32).astype(jnp.bfloat16)
    return momentum_new, roll_out
```

```python
import functools

import jax
import jax.numpy as jnp
from jax import lax
from jax.experimental import pallas as pl
from jax.experimental.pallas import tpu as pltpu
from jax.sharding import PartitionSpec as P

MOMENTUM = 0.9
LEARN_RATE = 0.002
SIDE = 4
ROWS = 256
SPANS = {"x": (0, 1024), "z": (1024, 768)}
OWNERS = ("grp", "fsdp")


def shift(v, dx, dz):
    pairs = [
        (x * SIDE + z, ((x + dx) % SIDE) * SIDE + (z + dz) % SIDE)
        for x in range(SIDE)
        for z in range(SIDE)
    ]
    return lax.ppermute(v, OWNERS, pairs)


def along(first, v, d):
    return shift(v, d, 0) if first == "x" else shift(v, 0, d)


def term_body(jobs, added, g_ref, c_ref, h_ref, *refs):
    del g_ref
    job = pl.program_id(0) // 2
    total = lax.dot_general(
        c_ref[...], h_ref[...], (((0,), (0,)), ((), ())), preferred_element_type=jnp.float32
    )
    for j in range(jobs):

        @pl.when(job == j)
        def _(j=j):
            out = refs[added + j]
            more = refs[j][0].astype(jnp.float32) if added else 0.0
            out[0] = (total + more).astype(out.dtype)


def terms(g, c, h, first, jobs, added=()):
    tokens = c.shape[0]
    start, width = SPANS[first]

    def block(i, g_ref):
        x, z = g_ref[0] // SIDE, g_ref[0] % SIDE
        j = i // 2
        off, half = jobs[-1]
        for k in range(len(jobs) - 1):
            off = jnp.where(j == k, jobs[k][0], off)
            half = jnp.where(j == k, jobs[k][1], half)
        other = 2 * half + i % 2
        if first == "x":
            return 0, lax.rem(x + off, SIDE) * SIDE + other
        return 0, other * SIDE + lax.rem(z + off, SIDE)

    tiles = [
        pl.BlockSpec((1, ROWS, width), lambda i, g_ref, j=j: (jnp.clip(i - 2 * j, 0, 1), 0, 0))
        for j in range(len(jobs))
    ]
    shape = jax.ShapeDtypeStruct((2, ROWS, width), jnp.bfloat16)
    return pl.pallas_call(
        functools.partial(term_body, len(jobs), len(added)),
        grid_spec=pltpu.PrefetchScalarGridSpec(
            num_scalar_prefetch=1,
            grid=(2 * len(jobs),),
            in_specs=[
                pl.BlockSpec((tokens, ROWS), block),
                pl.BlockSpec((pl.Element(tokens), pl.Element(width)), lambda i, g_ref: (0, start)),
                *(tiles if added else ()),
            ],
            out_specs=tiles,
        ),
        out_shape=[shape] * len(jobs),
        cost_estimate=pl.CostEstimate(
            flops=4 * len(jobs) * tokens * ROWS * width,
            bytes_accessed=2 * tokens * (4 * ROWS + width) + 8 * len(jobs) * ROWS * width,
            transcendentals=0,
        ),
        name=f"term_{first}_" + "_".join(f"{o}{p}" for o, p in jobs),
    )(g, c, h, *added)


def add(*values):
    return sum(v.astype(jnp.float32) for v in values)


def behind(v, *others):
    return lax.optimization_barrier((v, *others))[0]


def second_phase(g, first, low, high, far_up, far_down):
    second = "z" if first == "x" else "x"
    at = lax.bitwise_and(g[0], SIDE - 1) if second == "z" else lax.shift_right_logical(g[0], 2)
    mine = jnp.concatenate([add(low, far_up), add(high, far_down)]).astype(jnp.bfloat16)
    half = ROWS // 2

    def piece(off, part):
        rows = lax.dynamic_slice_in_dim(mine, lax.bitwise_and(at + off, SIDE - 1), 1, 0)[0]
        return rows[part * half : (part + 1) * half]

    up = along(second, piece(2, 0), 1)
    down = along(second, piece(2, 1), -1)
    own_up = along(second, piece(1, 1), 1)
    own_down = along(second, piece(3, 0), -1)
    up = along(second, add(piece(1, 0), up).astype(jnp.bfloat16), 1)
    down = along(second, add(piece(3, 1), down).astype(jnp.bfloat16), -1)
    return jnp.concatenate([add(piece(0, 0), own_down, up), add(piece(0, 1), own_up, down)])


def local(h, c, w, m, r):
    g = lax.axis_index(OWNERS).astype(jnp.int32).reshape(1)
    tokens, width = r.shape
    lots = lax.axis_size("tp")
    share = tokens // lots
    dot = functools.partial(lax.dot_general, preferred_element_type=jnp.float32)

    r = r.reshape(lots, 1, share, width)
    near = [r, shift(r, -1, 0), shift(r, -2, 0), shift(r, 1, 0)]
    px = terms(g, c, h, "x", ((2, 0), (2, 1)))
    far_up, far_down = along("x", px[0], 1), along("x", px[1], -1)
    own = jnp.concatenate([behind(v, px[1]) for v in near], axis=1).reshape(SIDE * tokens, width)
    held = [own, shift(own, 0, -1), shift(own, 0, -2), shift(own, 0, 1)]
    pz = terms(behind(g, own), c, h, "z", ((2, 0), (2, 1)))
    zfar_up, zfar_down = along("z", pz[0], 1), along("z", pz[1], -1)
    px = terms(behind(g, pz[0]), c, h, "x", ((1, 1), (3, 0)))
    near_up, near_down = along("x", px[0], 1), along("x", px[1], -1)

    held = jnp.concatenate([behind(v, px[0]) for v in held])
    plain = (w - (LEARN_RATE * MOMENTUM) * m).astype(jnp.bfloat16)
    seen = dot(held, h, (((1,), (1,)), ((), ())))
    base = dot(held, plain, (((1,), (1,)), ((), ())))
    sent = jnp.concatenate([seen, base], axis=1).astype(jnp.bfloat16)
    sent = sent.reshape(SIDE, lots, SIDE * share, -1).transpose(1, 0, 2, 3)
    sent = sent.reshape(lots, SIDE * SIDE * share, -1)
    got = lax.all_to_all(sent, "tp", 0, 0, tiled=True)

    px = terms(behind(g, sent), c, h, "x", ((1, 0), (3, 1)), (far_up, far_down))
    far_up, far_down = along("x", px[0], 1), along("x", px[1], -1)
    pz = terms(behind(g, px[0]), c, h, "z", ((1, 1), (3, 0)))
    znear_up, znear_down = along("z", pz[0], 1), along("z", pz[1], -1)
    pz = terms(behind(g, pz[0]), c, h, "z", ((1, 0), (3, 1)), (zfar_up, zfar_down))
    zfar_up, zfar_down = along("z", pz[0], 1), along("z", pz[1], -1)

    got = add(*(behind(got, pz[0])[k] for k in range(lots)))
    seen, base = got[:, : c.shape[0]].astype(jnp.bfloat16), got[:, c.shape[0] :]
    change = dot(seen, c, (((1,), (0,)), ((), ())))
    blocks = SIDE * SIDE
    here = (jnp.arange(blocks) == g[0])[None, :, None]
    spread = jnp.where(here, base[:, None, :], 0.0).reshape(change.shape)
    part = (spread - LEARN_RATE * change).astype(jnp.bfloat16)
    part = part.reshape(SIDE, SIDE * share, -1)
    moved = [part[0]] + [shift(part[d], 0, d) for d in (1, 2, 3)]
    px = terms(behind(g, part), c, h, "x", ((0, 0), (0, 1)), (near_down, near_up))
    pz = terms(behind(g, px[0]), c, h, "z", ((0, 0), (0, 1)), (znear_down, znear_up))
    part = add(*(behind(v, pz[0]) for v in moved)).astype(jnp.bfloat16).reshape(SIDE, share, -1)
    moved = [part[0]] + [shift(part[d], d, 0) for d in (1, 2, 3)]

    left = second_phase(g, "x", px[0], px[1], far_up, far_down)
    right = second_phase(g, "z", pz[0], pz[1], zfar_up, zfar_down)
    momentum_new = MOMENTUM * m + jnp.concatenate([left, right], axis=1)

    part = add(*moved).astype(jnp.bfloat16)
    part = jnp.broadcast_to(part[None], (lots, *part.shape))
    roll_out = lax.all_to_all(part, "tp", 0, 0, tiled=True).reshape(tokens, -1)
    return momentum_new, roll_out


def solution(mesh):
    placed = (
        P(("grp", "fsdp"), "tp"),
        P(("grp", "fsdp"), None),
        P(("grp", "fsdp"), "tp"),
        P(("grp", "fsdp"), "tp"),
        P(("grp", "fsdp"), "tp"),
    )
    return jax.shard_map(
        local,
        mesh=mesh,
        in_specs=placed,
        out_specs=(P(("grp", "fsdp"), "tp"), P(("grp", "fsdp"), None)),
        check_vma=False,
    )
```
